128 devices in a mesh: row: 16 (over z, y_hi, core), col: 8 (over x, y_lo).
Axes of the slice: x: 4, y: 4 (y_hi: 2, y_lo: 2; y = y_hi * 2 + y_lo), z: 4, core: 2. Of those that a mesh axis runs over, the one named last changes fastest.
Arguments:
- observed: int32 [4096, 32, 2048], P('row', None, 'col'), may hold values 0 or 1
- first_factor: float32 [4096, 256], P(('row', 'col')), may hold values from -1.35 to 1.35
- second_factor: float32 [2048, 256], P(('col', 'row')), may hold values from -1.35 to 1.35
- third_factor: float32 [32, 256], replicated, may hold values from -1.35 to 1.35
Outputs:
- first_out: float32 [4096, 256], P(('row', 'col'))
- second_out: float32 [2048, 256], P(('col', 'row'))
- third_out: float32 [32, 256], replicated
The draws below stay inside these ranges and needn't reach their ends.
All inputs are finite; a program needn't handle non-finite values. No bound on the sum of `observed` on one device may be relied on, other than what follows from the above.
Results may differ from the reference program's by a relative error of at most 0.0003.
Values sent between devices are 32-bit elements; how exact they have to be, the bound alone decides.
A program may use at most 128 MiB of HBM per device.

```python
import jax
import jax.numpy as jnp
from jax import lax

R = 256
I_DEV = 256
K = 32
STEPS = 2
I = 4096
J = 2048


def drawn_values(key, rows, width):
    values = jax.random.truncated_normal(key, -3.0, 3.0, (rows, width), jnp.float32)
    return jnp.clip(0.45 * values, -1.35, 1.35)


def draw_first_factor(key, part):
    return drawn_values(key, I, R)


def draw_second_factor(key, part):
    return drawn_values(key, J, R)


def draw_third_factor(key, part):
    return drawn_values(key, K, R)


def plant(values, stream_key, smallest, high):
    longest = values.shape.index(max(values.shape))
    spots = []
    for shift in (0, 1):
        where = [jax.random.randint(jax.random.fold_in(stream_key, axis), (), 0, length) for axis, length in enumerate(values.shape)]
        where[longest] = (where[longest] + shift) % values.shape[longest]
        spots.append(tuple(where))
    return values.at[spots[0]].set(smallest).at[spots[1]].set(high)


def setup_inputs(seed: int = 0) -> dict:
    arg_keys = jax.random.split(jax.random.key(seed), 5)
    observed = plant((jax.random.randint(arg_keys[0], (I, K, J), 0, 3) < 1).astype(jnp.int32), jax.random.fold_in(arg_keys[0], 1), 0, 1)
    first_factor = draw_first_factor(jax.random.fold_in(arg_keys[4], 71), 0)
    second_factor = draw_second_factor(jax.random.fold_in(arg_keys[4], 71), 0)
    third_factor = draw_third_factor(jax.random.fold_in(arg_keys[4], 71), 0)
    return {"observed": observed, "first_factor": first_factor, "second_factor": second_factor, "third_factor": third_factor}


step_rate = 48.0
highest = lax.Precision.HIGHEST


def partials(observed_block, rows_block, factor_two, factor_three):
    rows_here, depth_count, cols_here = observed_block.shape
    rank_width = factor_three.shape[1]
    paired = (rows_block[:, None, :] * factor_three[None, :, :]).reshape(rows_here * depth_count, rank_width)
    logits = lax.dot_general(paired, factor_two, (((1,), (1,)), ((), ())), precision=highest, preferred_element_type=jnp.float32)
    derivative = jax.nn.sigmoid(logits) - observed_block.reshape(rows_here * depth_count, cols_here).astype(logits.dtype)
    part_two = lax.dot_general(derivative, paired, (((0,), (0,)), ((), ())), precision=highest, preferred_element_type=jnp.float32)
    carried = jnp.dot(derivative, factor_two, precision=highest, preferred_element_type=jnp.float32)
    carried = carried.reshape(rows_here, depth_count, rank_width)
    part_one = jnp.sum(carried * factor_three[None, :, :], axis=1)
    part_three = jnp.sum(carried * rows_block[:, None, :], axis=0)
    return part_one, part_two, part_three


def reference(observed, first_factor, second_factor, third_factor):
    factor_one, factor_two, factor_three = first_factor, second_factor, third_factor
    for iteration in range(STEPS):
        def accumulate(totals, block_index):
            start = (block_index * I_DEV).astype(jnp.int32)
            rows_block = lax.dynamic_slice_in_dim(factor_one, start, I_DEV, 0)
            observed_block = lax.dynamic_slice_in_dim(observed, start, I_DEV, 0)
            part_one, part_two, part_three = partials(observed_block, rows_block, factor_two, factor_three)
            return (totals[0] + part_two, totals[1] + part_three), part_one

        start_totals = (jnp.zeros((J, R), jnp.float32), jnp.zeros((K, R), jnp.float32))
        blocks = jnp.arange(I // I_DEV, dtype=jnp.int32)
        (grad_two, grad_three), grad_one = lax.scan(accumulate, start_totals, blocks)
        grad_one = grad_one.reshape(I, R)
        factor_one = factor_one - (step_rate / (J * K)) * grad_one
        factor_two = factor_two - (step_rate / (I * K)) * grad_two
        factor_three = factor_three - (step_rate / (I * J)) * grad_three
    return (factor_one, factor_two, factor_three)
```

```python
import functools

import jax
import jax.numpy as jnp
from jax import lax
from jax.experimental import pallas as pl
from jax.experimental.pallas import tpu as pltpu
from jax.sharding import PartitionSpec as P

STEPS = 2
step_rate = 48.0
f32, bf16 = jnp.float32, jnp.bfloat16
MESH = pl.DeviceIdType.MESH
NT = (((1,), (1,)), ((), ()))
NN = (((1,), (0,)), ((), ()))
TN = (((0,), (0,)), ((), ()))
LANES = 128
SUBLANES = 8
CHUNK = 16


def dot(a, b, dims):
    return lax.dot_general(a, b, dims, preferred_element_type=f32)


def split(x):
    high = x.astype(bf16)
    return high, (x - high.astype(f32)).astype(bf16)


def kernel(
    n_row, n_col, rates,
    obs_hbm, a_in, b_in, c_in,
    a_out, b_out, c_out,
    obs, a_all, b_all, c_now, b_high, b_low,
    ga, ga_got, gb, gb_got, gc, gc_part, gc_got, gc_sum, c_new,
    pair0, pair1, der0, der1,
    obs_sem, a_send, a_recv, b_send, b_recv, ga_send, ga_recv, gb_send, gb_recv,
    c1_send, c1_recv, c2_send, c2_recv, c3_send, c3_recv,
):
    row, col = lax.axis_index("row"), lax.axis_index("col")
    rate_one, rate_two, rate_three = rates
    depth, rank = c_in.shape
    tiles = [(k, l) for k in range(depth // SUBLANES) for l in range(rank // LANES)]

    def to_col(src, dst, send, recv, peer):
        return pltpu.make_async_remote_copy(
            src_ref=src, dst_ref=dst, send_sem=send, recv_sem=recv,
            device_id={"col": peer}, device_id_type=MESH,
        )

    def to_row(src, dst, send, recv, peer):
        return pltpu.make_async_remote_copy(
            src_ref=src, dst_ref=dst, send_sem=send, recv_sem=recv,
            device_id={"row": peer}, device_id_type=MESH,
        )

    def col_peer(d):
        return lax.rem(col + d, n_col)

    def row_peer(d):
        return lax.rem(row + d, n_row)

    rows_here = a_in.shape[0]

    def obs_copy(block):
        part = pl.ds(pl.multiple_of(block * rows_here, rows_here), rows_here)
        return pltpu.make_async_copy(obs_hbm.at[part], obs.at[part], obs_sem.at[block])

    barrier = pltpu.get_barrier_semaphore()
    for d in range(1, n_row):
        pl.semaphore_signal(barrier, inc=1, device_id={"row": row_peer(d)}, device_id_type=MESH)
    for d in range(1, n_col):
        pl.semaphore_signal(barrier, inc=1, device_id={"col": col_peer(d)}, device_id_type=MESH)
    for d in range(n_col):
        obs_copy(col_peer(d)).start()
    pl.semaphore_wait(barrier, n_row + n_col - 2)

    def send_b(step, src):
        for d in range(1, n_row):
            to_row(src, b_all.at[step, row], b_send.at[step, d], b_recv.at[step, row], row_peer(d)).start()

    def send_a(step, src):
        for d in range(1, n_col):
            to_col(src, a_all.at[step, col], a_send.at[step, d], a_recv.at[step, col], col_peer(d)).start()

    def wait_a(step, block):
        here = a_all.at[step, block]
        to_col(here, here, a_send.at[step, 0], a_recv.at[step, block], col_peer(1)).wait_recv()

    send_b(0, b_in)
    send_a(0, a_in)
    a_all[0, col] = a_in[...]
    b_all[0, row] = b_in[...]
    c_now[...] = c_in[...]

    for step in range(STEPS):
        for d in range(1, n_row):
            here = b_all.at[step, row_peer(d)]
            to_row(here, here, b_send.at[step, 0], b_recv.at[step, row_peer(d)], row_peer(1)).wait_recv()
        high, low = split(0.5 * b_all[step].reshape(n_row * b_in.shape[0], rank))
        b_high[...], b_low[...] = high, low
        gb[step] = jnp.zeros(gb.shape[1:], f32)
        gc[...] = jnp.zeros(gc.shape, f32)

        def rows_of(block, half):
            return a_all[step, block, pl.ds(half * CHUNK, CHUNK), :]

        def front(block, half, pair, der):
            start = pl.multiple_of(block * rows_here + half * CHUNK, CHUNK)
            seen = obs[pl.ds(start, CHUNK)].reshape(CHUNK * depth, -1)
            paired = (rows_of(block, half)[:, None, :] * c_now[...][None]).reshape(CHUNK * depth, rank)
            p_high, p_low = split(paired)
            half_logits = (
                dot(p_high, b_high[...], NT) + dot(p_low, b_high[...], NT) + dot(p_high, b_low[...], NT)
            )
            d_high, d_low = split(jnp.tanh(half_logits) + (1.0 - 2.0 * seen.astype(f32)))
            pair[0], pair[1] = p_high, p_low
            der[0], der[1] = d_high, d_low

        def back(block, half, pair, der):
            p_high, p_low, d_high, d_low = pair[0], pair[1], der[0], der[1]
            part_b = dot(d_high, p_high, TN) + dot(d_high, p_low, TN) + dot(d_low, p_high, TN)
            carried = dot(d_high, b_high[...], NN) + dot(d_high, b_low[...], NN) + dot(d_low, b_high[...], NN)
            carried = carried.reshape(CHUNK, depth, rank)
            ga[step, block, pl.ds(half * CHUNK, CHUNK), :] = jnp.sum(carried * c_now[...][None], axis=1)
            gc[...] += jnp.sum(carried * rows_of(block, half)[:, None, :], axis=0)
            gb[step] += part_b.reshape(gb.shape[1:])

        def send_ga(d):
            owner = col_peer(d)
            to_col(
                ga.at[step, owner], ga_got.at[step, col], ga_send.at[step, d], ga_recv.at[step, col], owner
            ).start()

        if step == 0:
            obs_copy(col).wait()
        front(col, 0, pair0, der0)

        def block_body(d, carry):
            block, later = col_peer(d), col_peer(d + 1)
            wait_a(step, later)
            if step == 0:
                obs_copy(later).wait()
            front(block, 1, pair1, der1)
            back(block, 0, pair0, der0)
            front(later, 0, pair0, der0)
            back(block, 1, pair1, der1)

            @pl.when(d > 0)
            def _():
                send_ga(d)

            return carry

        lax.fori_loop(0, n_col - 1, block_body, 0)
        last = col_peer(n_col - 1)
        front(last, 1, pair1, der1)
        back(last, 0, pair0, der0)
        back(last, 1, pair1, der1)

        for t, (k, l) in enumerate(tiles):
            gc_part[step, t] = gc[k * SUBLANES : (k + 1) * SUBLANES, l * LANES : (l + 1) * LANES]
        for d in range(1, n_col):
            owner = col_peer(d)
            to_col(
                gc_part.at[step, owner], gc_got.at[step, col], c1_send.at[step, d], c1_recv.at[step, col], owner
            ).start()
        for d in range(1, n_row):
            owner = row_peer(d)
            to_row(
                gb.at[step, owner], gb_got.at[step, row], gb_send.at[step, d], gb_recv.at[step, row], owner
            ).start()
        send_ga(n_col - 1)

        total = gc_part[step, col]
        for d in range(1, n_col):
            here = gc_got.at[step, col_peer(d)]
            to_col(here, here, c1_send.at[step, 0], c1_recv.at[step, col_peer(d)], col_peer(1)).wait_recv()
            total = total + here[...]
        gc_sum[step, row] = total
        for d in range(1, n_row):
            here = gc_sum.at[step, row]
            to_row(here, here, c2_send.at[step, d], c2_recv.at[step, row], row_peer(d)).start()

        total = gb[step, row]
        for d in range(1, n_row):
            here = gb_got.at[step, row_peer(d)]
            to_row(here, here, gb_send.at[step, 0], gb_recv.at[step, row_peer(d)], row_peer(1)).wait_recv()
            total = total + here[...]
        updated = b_all[step, row] - rate_two * total
        if step + 1 < STEPS:
            b_all[step + 1, row] = updated
            send_b(step + 1, b_all.at[step + 1, row])
        else:
            b_out[...] = updated

        total = ga[step, col]
        for d in range(1, n_col):
            here = ga_got.at[step, col_peer(d)]
            to_col(here, here, ga_send.at[step, 0], ga_recv.at[step, col_peer(d)], col_peer(1)).wait_recv()
            total = total + here[...]
        updated = a_all[step, col] - rate_one * total
        if step + 1 < STEPS:
            a_all[step + 1, col] = updated
            send_a(step + 1, a_all.at[step + 1, col])
        else:
            a_out[...] = updated

        total = gc_sum[step, row]
        for d in range(1, n_row):
            here = gc_sum.at[step, row_peer(d)]
            to_row(here, here, c2_send.at[step, 0], c2_recv.at[step, row_peer(d)], row_peer(1)).wait_recv()
            total = total + here[...]
        for t, (k, l) in enumerate(tiles):
            gc_part[step + 1, t] = c_now[k * SUBLANES : (k + 1) * SUBLANES, l * LANES : (l + 1) * LANES]
        c_new[step, col] = gc_part[step + 1, col] - rate_three * total
        for d in range(1, n_col):
            here = c_new.at[step, col]
            to_col(here, here, c3_send.at[step, d], c3_recv.at[step, col], col_peer(d)).start()
        for d in range(1, n_col):
            here = c_new.at[step, col_peer(d)]
            to_col(here, here, c3_send.at[step, 0], c3_recv.at[step, col_peer(d)], col_peer(1)).wait_recv()
        target = c_out if step + 1 == STEPS else c_now
        for t, (k, l) in enumerate(tiles):
            target[k * SUBLANES : (k + 1) * SUBLANES, l * LANES : (l + 1) * LANES] = c_new[step, t]

    for step in range(STEPS):
        for d in range(1, n_col):
            to_col(ga.at[step, 0], ga.at[step, 0], ga_send.at[step, d], ga_recv.at[step, 0], col_peer(d)).wait_send()
            for part, sem in ((gc_part, c1_send), (c_new, c3_send)):
                here = part.at[step, 0]
                to_col(here, here, sem.at[step, d], c1_recv.at[step, 0], col_peer(d)).wait_send()
            here = a_all.at[step, 0]
            to_col(here, here, a_send.at[step, d], a_recv.at[step, 0], col_peer(d)).wait_send()
        for d in range(1, n_row):
            for part, sem in ((gb, gb_send), (gc_sum, c2_send), (b_all, b_send)):
                here = part.at[step, 0]
                to_row(here, here, sem.at[step, d], gb_recv.at[step, 0], row_peer(d)).wait_send()


def per_device(observed, first_factor, second_factor, third_factor):
    n_row, n_col = lax.axis_size("row"), lax.axis_size("col")
    first_here, depth, second_here = observed.shape
    rank = third_factor.shape[1]
    rates = (
        step_rate / (second_here * n_col * depth),
        0.5 * step_rate / (first_here * n_row * depth),
        step_rate / (first_here * n_row * second_here * n_col),
    )
    a_rows, b_rows = first_factor.shape[0], second_factor.shape[0]
    tile = (SUBLANES, LANES)
    dma = pltpu.SemaphoreType.DMA
    vmem = pl.BlockSpec(memory_space=pltpu.VMEM)
    return pl.pallas_call(
        functools.partial(kernel, n_row, n_col, rates),
        name="cp_steps",
        out_shape=[
            jax.ShapeDtypeStruct(first_factor.shape, f32),
            jax.ShapeDtypeStruct(second_factor.shape, f32),
            jax.ShapeDtypeStruct(third_factor.shape, f32),
        ],
        in_specs=[pl.BlockSpec(memory_space=pl.ANY), vmem, vmem, vmem],
        out_specs=[vmem] * 3,
        scratch_shapes=[
            pltpu.VMEM(observed.shape, jnp.int32),
            pltpu.VMEM((STEPS, n_col, a_rows, rank), f32),
            pltpu.VMEM((STEPS, n_row, b_rows, rank), f32),
            pltpu.VMEM((depth, rank), f32),
            pltpu.VMEM((second_here, rank), bf16),
            pltpu.VMEM((second_here, rank), bf16),
            pltpu.VMEM((STEPS, n_col, a_rows, rank), f32),
            pltpu.VMEM((STEPS, n_col, a_rows, rank), f32),
            pltpu.VMEM((STEPS, n_row, b_rows, rank), f32),
            pltpu.VMEM((STEPS, n_row, b_rows, rank), f32),
            pltpu.VMEM((depth, rank), f32),
            pltpu.VMEM((STEPS + 1, n_col, *tile), f32),
            pltpu.VMEM((STEPS, n_col, *tile), f32),
            pltpu.VMEM((STEPS, n_row, *tile), f32),
            pltpu.VMEM((STEPS, n_col, *tile), f32),
            pltpu.VMEM((2, CHUNK * depth, rank), bf16),
            pltpu.VMEM((2, CHUNK * depth, rank), bf16),
            pltpu.VMEM((2, CHUNK * depth, second_here), bf16),
            pltpu.VMEM((2, CHUNK * depth, second_here), bf16),
            dma((n_col,)),
        ]
        + [dma((STEPS, n)) for n in (n_col, n_row, n_col, n_row, n_col, n_row, n_col) for _ in range(2)],
        compiler_params=pltpu.CompilerParams(
            collective_id=0, has_side_effects=True, vmem_limit_bytes=62 * 2**20
        ),
    )(observed, first_factor, second_factor, third_factor)


def solution(mesh):
    return jax.shard_map(
        per_device,
        mesh=mesh,
        in_specs=(P("row", None, "col"), P(("row", "col"), None), P(("col", "row"), None), P()),
        out_specs=(P(("row", "col"), None), P(("col", "row"), None), P()),
        check_vma=False,
    )
```

```python
import functools

import jax
import jax.numpy as jnp
from jax import lax
from jax.experimental import pallas as pl
from jax.experimental.pallas import tpu as pltpu
from jax.sharding import PartitionSpec as P

STEPS = 2
step_rate = 48.0
f32, bf16 = jnp.float32, jnp.bfloat16
MESH = pl.DeviceIdType.MESH
NN = (((1,), (0,)), ((), ()))
TN = (((0,), (0,)), ((), ()))
LANES = 128
SUBLANES = 8
MIDDLE = ("b", "a", "c")
CHUNK = 16


def dot(a, b, dims):
    return lax.dot_general(a, b, dims, preferred_element_type=f32)


def split(x):
    high = x.astype(bf16)
    return high, (x - high.astype(f32)).astype(bf16)


def kernel(
    n_row, n_col, rates,
    obs_hbm, a_in, b_in, c_in,
    a_out, b_out, c_out,
    obs, a_all, b_all, c_now, b_high, b_low, bt_high, bt_low,
    ga, ga_got, gb, gb_got, gc, gc_part, gc_got, gc_sum, c_new, c_tile,
    pair0, pair1, der0, der1,
    obs_sem, a_send, a_recv, b_send, b_recv, ga_send, ga_recv, gb_send, gb_recv,
    c1_send, c1_recv, c2_send, c2_recv, c3_send, c3_recv,
):
    row, col = lax.axis_index("row"), lax.axis_index("col")
    rate_one, rate_two, rate_three = rates
    depth, rank = c_in.shape
    tiles = [(k, l) for k in range(depth // SUBLANES) for l in range(rank // LANES)]

    def to_col(src, dst, send, recv, peer):
        return pltpu.make_async_remote_copy(
            src_ref=src, dst_ref=dst, send_sem=send, recv_sem=recv,
            device_id={"col": peer}, device_id_type=MESH,
        )

    def to_row(src, dst, send, recv, peer):
        return pltpu.make_async_remote_copy(
            src_ref=src, dst_ref=dst, send_sem=send, recv_sem=recv,
            device_id={"row": peer}, device_id_type=MESH,
        )

    def col_peer(d):
        return lax.rem(col + d, n_col)

    def row_peer(d):
        return lax.rem(row + d, n_row)

    rows_here = a_in.shape[0]

    def obs_copy(block):
        part = pl.ds(pl.multiple_of(block * rows_here, rows_here), rows_here)
        return pltpu.make_async_copy(obs_hbm.at[part], obs.at[part], obs_sem.at[block])

    barrier = pltpu.get_barrier_semaphore()
    for d in range(1, n_row):
        pl.semaphore_signal(barrier, inc=1, device_id={"row": row_peer(d)}, device_id_type=MESH)
    for d in range(1, n_col):
        pl.semaphore_signal(barrier, inc=1, device_id={"col": col_peer(d)}, device_id_type=MESH)
    for d in range(n_col):
        obs_copy(col_peer(d)).start()
    pl.semaphore_wait(barrier, n_row + n_col - 2)

    def send_b(step, src):
        for d in range(1, n_row):
            to_row(src, b_all.at[step, row], b_send.at[step, d], b_recv.at[step, row], row_peer(d)).start()

    def send_a(step, src):
        for d in reversed(range(1, n_col)):
            to_col(src, a_all.at[step, col], a_send.at[step, d], a_recv.at[step, col], col_peer(d)).start()

    def wait_a(step, block):
        here = a_all.at[step, block]
        to_col(here, here, a_send.at[step, 0], a_recv.at[step, block], col_peer(1)).wait_recv()

    send_b(0, b_in)
    send_a(0, a_in)
    a_all[0, col] = a_in[...]
    b_all[0, row] = b_in[...]
    c_now[...] = c_in[...]

    def all_left(step):
        for d in range(1, n_col):
            for part, sem in ((ga, ga_send), (gc_part, c1_send), (c_new, c3_send)):
                here = part.at[step, 0]
                to_col(here, here, sem.at[step, d], a_recv.at[step, 0], col_peer(d)).wait_send()
        for d in range(1, n_row):
            for part, sem in ((gb, gb_send), (gc_sum, c2_send)):
                here = part.at[step, 0]
                to_row(here, here, sem.at[step, d], gb_recv.at[step, 0], row_peer(d)).wait_send()

    for step in range(STEPS):
        for d in range(1, n_row):
            here = b_all.at[step, row_peer(d)]
            to_row(here, here, b_send.at[step, 0], b_recv.at[step, row_peer(d)], row_peer(1)).wait_recv()
        halved = 0.5 * b_all[step].reshape(n_row * b_in.shape[0], rank)
        b_high[...], b_low[...] = split(halved)
        bt_high[...], bt_low[...] = split(halved.T)
        gb[step] = jnp.zeros(gb.shape[1:], f32)
        gc[...] = jnp.zeros(gc.shape, f32)

        def rows_of(block, half):
            return a_all[step, block, pl.ds(half * CHUNK, CHUNK), :]

        def front(block, half, pair, der):
            start = pl.multiple_of(block * rows_here + half * CHUNK, CHUNK)
            seen = obs[pl.ds(start, CHUNK)].reshape(CHUNK * depth, -1)
            paired = (rows_of(block, half)[:, None, :] * c_now[...][None]).reshape(CHUNK * depth, rank)
            p_high, p_low = split(paired)
            half_logits = (
                dot(p_high, bt_high[...], NN) + dot(p_low, bt_high[...], NN) + dot(p_high, bt_low[...], NN)
            )
            d_high, d_low = split(jnp.tanh(half_logits) + (1.0 - 2.0 * seen.astype(f32)))
            pair[0], pair[1] = p_high, p_low
            der[0], der[1] = d_high, d_low

        def back(block, half, pair, der):
            p_high, p_low, d_high, d_low = pair[0], pair[1], der[0], der[1]
            part_b = dot(d_high, p_high, TN) + dot(d_high, p_low, TN) + dot(d_low, p_high, TN)
            carried = dot(d_high, b_high[...], NN) + dot(d_high, b_low[...], NN) + dot(d_low, b_high[...], NN)
            carried = carried.reshape(CHUNK, depth, rank)
            ga[step, block, pl.ds(half * CHUNK, CHUNK), :] = jnp.sum(carried * c_now[...][None], axis=1)
            gc[...] += jnp.sum(carried * rows_of(block, half)[:, None, :], axis=0)
            gb[step] += part_b.reshape(gb.shape[1:])

        def send_ga(d):
            owner = col_peer(d)
            to_col(
                ga.at[step, owner], ga_got.at[step, col], ga_send.at[step, d], ga_recv.at[step, col], owner
            ).start()

        if step == 0:
            obs_copy(col).wait()
        front(col, 0, pair0, der0)

        def block_body(d, carry):
            block, later = col_peer(d), col_peer(d + 1)
            wait_a(step, later)
            if step == 0:
                obs_copy(later).wait()
            front(block, 1, pair1, der1)
            back(block, 0, pair0, der0)
            front(later, 0, pair0, der0)
            back(block, 1, pair1, der1)

            @pl.when(d > 0)
            def _():
                send_ga(d)

            return carry

        lax.fori_loop(0, n_col - 1, block_body, 0)
        last = col_peer(n_col - 1)
        front(last, 1, pair1, der1)
        back(last, 0, pair0, der0)
        back(last, 1, pair1, der1)

        for t, (k, l) in enumerate(tiles):
            gc_part[step, t] = gc[k * SUBLANES : (k + 1) * SUBLANES, l * LANES : (l + 1) * LANES]
            c_tile[t] = c_now[k * SUBLANES : (k + 1) * SUBLANES, l * LANES : (l + 1) * LANES]
        for d in range(1, n_col):
            owner = col_peer(d)
            to_col(
                gc_part.at[step, owner], gc_got.at[step, col], c1_send.at[step, d], c1_recv.at[step, col], owner
            ).start()
        gc_got[step, col] = gc_part[step, col]
        final = step + 1 == STEPS

        def send_gb():
            for d in range(1, n_row):
                owner = row_peer(d)
                to_row(
                    gb.at[step, owner], gb_got.at[step, row], gb_send.at[step, d], gb_recv.at[step, row], owner
                ).start()
            send_ga(n_col - 1)

        if not final:
            send_gb()
        for d in range(1, n_col):
            here = gc_got.at[step, col_peer(d)]
            to_col(here, here, c1_send.at[step, 0], c1_recv.at[step, col_peer(d)], col_peer(1)).wait_recv()
        gc_sum[step, row] = sum(gc_got[step, p] for p in range(n_col))
        for d in range(1, n_row):
            here = gc_sum.at[step, row]
            to_row(here, here, c2_send.at[step, d], c2_recv.at[step, row], row_peer(d)).start()
        if final:
            send_gb()
            for earlier in range(STEPS):
                for d in range(1, n_col):
                    here = a_all.at[earlier, 0]
                    to_col(here, here, a_send.at[earlier, d], a_recv.at[earlier, 0], col_peer(d)).wait_send()
                for d in range(1, n_row):
                    here = b_all.at[earlier, 0]
                    to_row(here, here, b_send.at[earlier, d], b_recv.at[earlier, 0], row_peer(d)).wait_send()
            for earlier in range(STEPS - 1):
                all_left(earlier)

        def update_a():
            total = ga[step, col]
            for d in range(1, n_col):
                here = ga_got.at[step, col_peer(d)]
                to_col(here, here, ga_send.at[step, 0], ga_recv.at[step, col_peer(d)], col_peer(1)).wait_recv()
                total = total + here[...]
            updated = a_all[step, col] - rate_one * total
            if final:
                a_out[...] = updated
            else:
                a_all[step + 1, col] = updated
                send_a(step + 1, a_all.at[step + 1, col])

        def update_b():
            total = gb[step, row]
            for d in range(1, n_row):
                here = gb_got.at[step, row_peer(d)]
                to_row(here, here, gb_send.at[step, 0], gb_recv.at[step, row_peer(d)], row_peer(1)).wait_recv()
                total = total + here[...]
            updated = b_all[step, row] - rate_two * total
            if final:
                b_out[...] = updated
            else:
                b_all[step + 1, row] = updated
                send_b(step + 1, b_all.at[step + 1, row])

        def finish_c():
            for d in range(1, n_row):
                here = gc_sum.at[step, row_peer(d)]
                to_row(here, here, c2_send.at[step, 0], c2_recv.at[step, row_peer(d)], row_peer(1)).wait_recv()
            total = sum(gc_sum[step, p] for p in range(n_row))
            c_new[step, col] = c_tile[col] - rate_three * total
            for d in range(1, n_col):
                here = c_new.at[step, col]
                to_col(here, here, c3_send.at[step, d], c3_recv.at[step, col], col_peer(d)).start()

        for stage in MIDDLE if not final else ("c", "b", "a"):
            {"a": update_a, "b": update_b, "c": finish_c}[stage]()
        if final:
            all_left(step)
        for d in range(1, n_col):
            here = c_new.at[step, col_peer(d)]
            to_col(here, here, c3_send.at[step, 0], c3_recv.at[step, col_peer(d)], col_peer(1)).wait_recv()
        target = c_out if final else c_now
        for t, (k, l) in enumerate(tiles):
            target[k * SUBLANES : (k + 1) * SUBLANES, l * LANES : (l + 1) * LANES] = c_new[step, t]


def hand_over(*refs):
    n = len(refs) // 2
    for source, target in zip(refs[:n], refs[n:]):
        target[...] = source[...]


def per_device(observed, first_factor, second_factor, third_factor):
    n_row, n_col = lax.axis_size("row"), lax.axis_size("col")
    first_here, depth, second_here = observed.shape
    rank = third_factor.shape[1]
    rates = (
        step_rate / (second_here * n_col * depth),
        0.5 * step_rate / (first_here * n_row * depth),
        step_rate / (first_here * n_row * second_here * n_col),
    )
    a_rows, b_rows = first_factor.shape[0], second_factor.shape[0]
    tile = (SUBLANES, LANES)
    dma = pltpu.SemaphoreType.DMA
    vmem = pl.BlockSpec(memory_space=pltpu.VMEM)
    results = [jax.ShapeDtypeStruct(x.shape, f32) for x in (first_factor, second_factor, third_factor)]
    factors = pl.pallas_call(
        functools.partial(kernel, n_row, n_col, rates),
        name="cp_steps",
        out_shape=results,
        in_specs=[pl.BlockSpec(memory_space=pl.ANY), vmem, vmem, vmem],
        out_specs=[vmem] * 3,
        scratch_shapes=[
            pltpu.VMEM(observed.shape, jnp.int32),
            pltpu.VMEM((STEPS, n_col, a_rows, rank), f32),
            pltpu.VMEM((STEPS, n_row, b_rows, rank), f32),
            pltpu.VMEM((depth, rank), f32),
            pltpu.VMEM((second_here, rank), bf16),
            pltpu.VMEM((second_here, rank), bf16),
            pltpu.VMEM((rank, second_here), bf16),
            pltpu.VMEM((rank, second_here), bf16),
            pltpu.VMEM((STEPS, n_col, a_rows, rank), f32),
            pltpu.VMEM((STEPS, n_col, a_rows, rank), f32),
            pltpu.VMEM((STEPS, n_row, b_rows, rank), f32),
            pltpu.VMEM((STEPS, n_row, b_rows, rank), f32),
            pltpu.VMEM((depth, rank), f32),
            pltpu.VMEM((STEPS, n_col, *tile), f32),
            pltpu.VMEM((STEPS, n_col, *tile), f32),
            pltpu.VMEM((STEPS, n_row, *tile), f32),
            pltpu.VMEM((STEPS, n_col, *tile), f32),
            pltpu.VMEM((n_col, *tile), f32),
            pltpu.VMEM((2, CHUNK * depth, rank), bf16),
            pltpu.VMEM((2, CHUNK * depth, rank), bf16),
            pltpu.VMEM((2, CHUNK * depth, second_here), bf16),
            pltpu.VMEM((2, CHUNK * depth, second_here), bf16),
            dma((n_col,)),
        ]
        + [dma((STEPS, n)) for n in (n_col, n_row, n_col, n_row, n_col, n_row, n_col) for _ in range(2)],
        compiler_params=pltpu.CompilerParams(
            collective_id=0, has_side_effects=True, vmem_limit_bytes=62 * 2**20
        ),
    )(observed, first_factor, second_factor, third_factor)
    give = pl.pallas_call(hand_over, name="hand_over", out_shape=results, in_specs=[vmem] * 3, out_specs=[vmem] * 3)
    return tuple(give(*factors))


def solution(mesh):
    return jax.shard_map(
        per_device,
        mesh=mesh,
        in_specs=(P("row", None, "col"), P(("row", "col"), None), P(("col", "row"), None), P()),
        out_specs=(P(("row", "col"), None), P(("col", "row"), None), P()),
        check_vma=False,
    )
```

```python
import functools

import jax
import jax.numpy as jnp
from jax import lax
from jax.experimental import pallas as pl
from jax.experimental.pallas import tpu as pltpu
from jax.sharding import PartitionSpec as P

STEPS = 2
step_rate = 48.0
f32, bf16 = jnp.float32, jnp.bfloat16
MESH = pl.DeviceIdType.MESH
NN = (((1,), (0,)), ((), ()))
TN = (((0,), (0,)), ((), ()))
LANES = 128
SUBLANES = 8
MIDDLE = ("b", "a", "c")
CHUNK = 16


def dot(a, b, dims):
    return lax.dot_general(a, b, dims, preferred_element_type=f32)


def split(x):
    high = x.astype(bf16)
    return high, (x - high.astype(f32)).astype(bf16)


def kernel(
    n_row, n_col, rates,
    obs_hbm, a_in, b_in, c_in,
    a_out, b_out, c_out,
    obs, a_all, b_all, c_now, b_high, b_low, bt_high, bt_low,
    ga, ga_got, gb, gb_got, gc, gc_part, gc_got, gc_sum, c_new, c_tile,
    pair0, pair1, der0, der1,
    obs_sem, own_sem, a_send, a_recv, b_send, b_recv, ga_send, ga_recv, gb_send, gb_recv,
    c1_send, c1_recv, c2_send, c2_recv, c3_send, c3_recv,
):
    row, col = lax.axis_index("row"), lax.axis_index("col")
    rate_one, rate_two, rate_three = rates
    depth, rank = c_in.shape
    tiles = [(k, l) for k in range(depth // SUBLANES) for l in range(rank // LANES)]

    def to_col(src, dst, send, recv, peer):
        return pltpu.make_async_remote_copy(
            src_ref=src, dst_ref=dst, send_sem=send, recv_sem=recv,
            device_id={"col": peer}, device_id_type=MESH,
        )

    def to_row(src, dst, send, recv, peer):
        return pltpu.make_async_remote_copy(
            src_ref=src, dst_ref=dst, send_sem=send, recv_sem=recv,
            device_id={"row": peer}, device_id_type=MESH,
        )

    def col_peer(d):
        return lax.rem(col + d, n_col)

    def row_peer(d):
        return lax.rem(row + d, n_row)

    rows_here = a_in.shape[0]

    def obs_copy(block):
        part = pl.ds(pl.multiple_of(block * rows_here, rows_here), rows_here)
        return pltpu.make_async_copy(obs_hbm.at[part], obs.at[part], obs_sem.at[block])

    barrier = pltpu.get_barrier_semaphore()
    for d in range(1, n_row):
        pl.semaphore_signal(barrier, inc=1, device_id={"row": row_peer(d)}, device_id_type=MESH)
    for d in range(1, n_col):
        pl.semaphore_signal(barrier, inc=1, device_id={"col": col_peer(d)}, device_id_type=MESH)
    own = [
        pltpu.make_async_copy(b_in, b_all.at[0, row], own_sem.at[0]),
        pltpu.make_async_copy(a_in, a_all.at[0, col], own_sem.at[1]),
        pltpu.make_async_copy(c_in, c_now, own_sem.at[2]),
    ]
    for copy in own:
        copy.start()
    for d in range(n_col):
        obs_copy(col_peer(d)).start()
    for copy in own:
        copy.wait()
    pl.semaphore_wait(barrier, n_row + n_col - 2)

    def send_b(step, src):
        for d in range(1, n_row):
            to_row(src, b_all.at[step, row], b_send.at[step, d], b_recv.at[step, row], row_peer(d)).start()

    def send_a(step, src):
        for d in reversed(range(1, n_col)):
            to_col(src, a_all.at[step, col], a_send.at[step, d], a_recv.at[step, col], col_peer(d)).start()

    def wait_a(step, block):
        here = a_all.at[step, block]
        to_col(here, here, a_send.at[step, 0], a_recv.at[step, block], col_peer(1)).wait_recv()

    send_b(0, b_all.at[0, row])
    send_a(0, a_all.at[0, col])

    def c_arrived(step):
        for d in range(1, n_col):
            here = c_new.at[step, col_peer(d)]
            to_col(here, here, c3_send.at[step, 0], c3_recv.at[step, col_peer(d)], col_peer(1)).wait_recv()
        target = c_out if step + 1 == STEPS else c_now
        for t, (k, l) in enumerate(tiles):
            target[k * SUBLANES : (k + 1) * SUBLANES, l * LANES : (l + 1) * LANES] = c_new[step, t]

    def all_left(step):
        for d in range(1, n_col):
            for part, sem in ((ga, ga_send), (gc_part, c1_send), (c_new, c3_send)):
                here = part.at[step, 0]
                to_col(here, here, sem.at[step, d], a_recv.at[step, 0], col_peer(d)).wait_send()
        for d in range(1, n_row):
            for part, sem in ((gb, gb_send), (gc_sum, c2_send)):
                here = part.at[step, 0]
                to_row(here, here, sem.at[step, d], gb_recv.at[step, 0], row_peer(d)).wait_send()

    for step in range(STEPS):
        gb[step] = jnp.zeros(gb.shape[1:], f32)
        gc[...] = jnp.zeros(gc.shape, f32)
        for d in range(1, n_row):
            here = b_all.at[step, row_peer(d)]
            to_row(here, here, b_send.at[step, 0], b_recv.at[step, row_peer(d)], row_peer(1)).wait_recv()
        halved = 0.5 * b_all[step].reshape(n_row * b_in.shape[0], rank)
        b_high[...], b_low[...] = split(halved)
        bt_high[...], bt_low[...] = split(halved.T)

        def rows_of(block, half):
            return a_all[step, block, pl.ds(half * CHUNK, CHUNK), :]

        def front(block, half, pair, der):
            start = pl.multiple_of(block * rows_here + half * CHUNK, CHUNK)
            seen = obs[pl.ds(start, CHUNK)].reshape(CHUNK * depth, -1)
            paired = (rows_of(block, half)[:, None, :] * c_now[...][None]).reshape(CHUNK * depth, rank)
            p_high, p_low = split(paired)
            half_logits = (
                dot(p_high, bt_high[...], NN) + dot(p_low, bt_high[...], NN) + dot(p_high, bt_low[...], NN)
            )
            d_high, d_low = split(jnp.tanh(half_logits) + (1.0 - 2.0 * seen.astype(f32)))
            pair[0], pair[1] = p_high, p_low
            der[0], der[1] = d_high, d_low

        def back(block, half, pair, der):
            p_high, p_low, d_high, d_low = pair[0], pair[1], der[0], der[1]
            part_b = dot(d_high, p_high, TN) + dot(d_high, p_low, TN) + dot(d_low, p_high, TN)
            carried = dot(d_high, b_high[...], NN) + dot(d_high, b_low[...], NN) + dot(d_low, b_high[...], NN)
            carried = carried.reshape(CHUNK, depth, rank)
            ga[step, block, pl.ds(half * CHUNK, CHUNK), :] = jnp.sum(carried * c_now[...][None], axis=1)
            gc[...] += jnp.sum(carried * rows_of(block, half)[:, None, :], axis=0)
            gb[step] += part_b.reshape(gb.shape[1:])

        def send_ga(d):
            owner = col_peer(d)
            to_col(
                ga.at[step, owner], ga_got.at[step, col], ga_send.at[step, d], ga_recv.at[step, col], owner
            ).start()

        if step == 0:
            obs_copy(col).wait()
        else:
            c_arrived(step - 1)
        front(col, 0, pair0, der0)

        def block_body(d, carry):
            block, later = col_peer(d), col_peer(d + 1)
            wait_a(step, later)
            if step == 0:
                obs_copy(later).wait()
            front(block, 1, pair1, der1)
            back(block, 0, pair0, der0)
            front(later, 0, pair0, der0)
            back(block, 1, pair1, der1)

            @pl.when(d > 0)
            def _():
                send_ga(d)

            return carry

        lax.fori_loop(0, n_col - 1, block_body, 0)
        last = col_peer(n_col - 1)
        front(last, 1, pair1, der1)
        back(last, 0, pair0, der0)
        back(last, 1, pair1, der1)

        for t, (k, l) in enumerate(tiles):
            gc_part[step, t] = gc[k * SUBLANES : (k + 1) * SUBLANES, l * LANES : (l + 1) * LANES]
            c_tile[t] = c_now[k * SUBLANES : (k + 1) * SUBLANES, l * LANES : (l + 1) * LANES]
        for d in range(1, n_col):
            owner = col_peer(d)
            to_col(
                gc_part.at[step, owner], gc_got.at[step, col], c1_send.at[step, d], c1_recv.at[step, col], owner
            ).start()
        gc_got[step, col] = gc_part[step, col]
        final = step + 1 == STEPS

        def send_gb():
            for d in range(1, n_row):
                owner = row_peer(d)
                to_row(
                    gb.at[step, owner], gb_got.at[step, row], gb_send.at[step, d], gb_recv.at[step, row], owner
                ).start()
            send_ga(n_col - 1)

        if not final:
            send_gb()
        for d in range(1, n_col):
            here = gc_got.at[step, col_peer(d)]
            to_col(here, here, c1_send.at[step, 0], c1_recv.at[step, col_peer(d)], col_peer(1)).wait_recv()
        gc_sum[step, row] = sum(gc_got[step, p] for p in range(n_col))
        for d in range(1, n_row):
            here = gc_sum.at[step, row]
            to_row(here, here, c2_send.at[step, d], c2_recv.at[step, row], row_peer(d)).start()
        if final:
            send_gb()
            for earlier in range(STEPS):
                for d in range(1, n_col):
                    here = a_all.at[earlier, 0]
                    to_col(here, here, a_send.at[earlier, d], a_recv.at[earlier, 0], col_peer(d)).wait_send()
                for d in range(1, n_row):
                    here = b_all.at[earlier, 0]
                    to_row(here, here, b_send.at[earlier, d], b_recv.at[earlier, 0], row_peer(d)).wait_send()
            for earlier in range(STEPS - 1):
                all_left(earlier)

        def update_a():
            total = ga[step, col]
            for d in range(1, n_col):
                here = ga_got.at[step, col_peer(d)]
                to_col(here, here, ga_send.at[step, 0], ga_recv.at[step, col_peer(d)], col_peer(1)).wait_recv()
                total = total + here[...]
            updated = a_all[step, col] - rate_one * total
            if final:
                a_out[...] = updated
            else:
                a_all[step + 1, col] = updated
                send_a(step + 1, a_all.at[step + 1, col])

        def update_b():
            total = gb[step, row]
            for d in range(1, n_row):
                here = gb_got.at[step, row_peer(d)]
                to_row(here, here, gb_send.at[step, 0], gb_recv.at[step, row_peer(d)], row_peer(1)).wait_recv()
                total = total + here[...]
            updated = b_all[step, row] - rate_two * total
            if final:
                b_out[...] = updated
            else:
                b_all[step + 1, row] = updated
                send_b(step + 1, b_all.at[step + 1, row])

        def finish_c():
            for d in range(1, n_row):
                here = gc_sum.at[step, row_peer(d)]
                to_row(here, here, c2_send.at[step, 0], c2_recv.at[step, row_peer(d)], row_peer(1)).wait_recv()
            total = sum(gc_sum[step, p] for p in range(n_row))
            c_new[step, col] = c_tile[col] - rate_three * total
            for d in range(1, n_col):
                here = c_new.at[step, col]
                to_col(here, here, c3_send.at[step, d], c3_recv.at[step, col], col_peer(d)).start()

        for stage in MIDDLE if not final else ("c", "b", "a"):
            {"a": update_a, "b": update_b, "c": finish_c}[stage]()
        if final:
            all_left(step)
        if final:
            c_arrived(step)


def hand_over(*refs):
    n = len(refs) // 2
    for source, target in zip(refs[:n], refs[n:]):
        target[...] = source[...]


def per_device(observed, first_factor, second_factor, third_factor):
    n_row, n_col = lax.axis_size("row"), lax.axis_size("col")
    first_here, depth, second_here = observed.shape
    rank = third_factor.shape[1]
    rates = (
        step_rate / (second_here * n_col * depth),
        0.5 * step_rate / (first_here * n_row * depth),
        step_rate / (first_here * n_row * second_here * n_col),
    )
    a_rows, b_rows = first_factor.shape[0], second_factor.shape[0]
    tile = (SUBLANES, LANES)
    dma = pltpu.SemaphoreType.DMA
    vmem = pl.BlockSpec(memory_space=pltpu.VMEM)
    results = [jax.ShapeDtypeStruct(x.shape, f32) for x in (first_factor, second_factor, third_factor)]
    factors = pl.pallas_call(
        functools.partial(kernel, n_row, n_col, rates),
        name="cp_steps",
        out_shape=results,
        in_specs=[pl.BlockSpec(memory_space=pl.ANY)] * 4,
        out_specs=[vmem] * 3,
        scratch_shapes=[
            pltpu.VMEM(observed.shape, jnp.int32),
            pltpu.VMEM((STEPS, n_col, a_rows, rank), f32),
            pltpu.VMEM((STEPS, n_row, b_rows, rank), f32),
            pltpu.VMEM((depth, rank), f32),
            pltpu.VMEM((second_here, rank), bf16),
            pltpu.VMEM((second_here, rank), bf16),
            pltpu.VMEM((rank, second_here), bf16),
            pltpu.VMEM((rank, second_here), bf16),
            pltpu.VMEM((STEPS, n_col, a_rows, rank), f32),
            pltpu.VMEM((STEPS, n_col, a_rows, rank), f32),
            pltpu.VMEM((STEPS, n_row, b_rows, rank), f32),
            pltpu.VMEM((STEPS, n_row, b_rows, rank), f32),
            pltpu.VMEM((depth, rank), f32),
            pltpu.VMEM((STEPS, n_col, *tile), f32),
            pltpu.VMEM((STEPS, n_col, *tile), f32),
            pltpu.VMEM((STEPS, n_row, *tile), f32),
            pltpu.VMEM((STEPS, n_col, *tile), f32),
            pltpu.VMEM((n_col, *tile), f32),
            pltpu.VMEM((2, CHUNK * depth, rank), bf16),
            pltpu.VMEM((2, CHUNK * depth, rank), bf16),
            pltpu.VMEM((2, CHUNK * depth, second_here), bf16),
            pltpu.VMEM((2, CHUNK * depth, second_here), bf16),
            dma((n_col,)),
            dma((3,)),
        ]
        + [dma((STEPS, n)) for n in (n_col, n_row, n_col, n_row, n_col, n_row, n_col) for _ in range(2)],
        compiler_params=pltpu.CompilerParams(
            collective_id=0, has_side_effects=True, vmem_limit_bytes=62 * 2**20
        ),
    )(observed, first_factor, second_factor, third_factor)
    give = pl.pallas_call(hand_over, name="hand_over", out_shape=results, in_specs=[vmem] * 3, out_specs=[vmem] * 3)
    return tuple(give(*factors))


def solution(mesh):
    return jax.shard_map(
        per_device,
        mesh=mesh,
        in_specs=(P("row", None, "col"), P(("row", "col"), None), P(("col", "row"), None), P()),
        out_specs=(P(("row", "col"), None), P(("col", "row"), None), P()),
        check_vma=False,
    )
```
